32 devices in a mesh: view: 4 (over x, core), pencil: 8 (over z, y).
Axes of the slice: x: 2, y: 2, z: 4, core: 2. Of those that a mesh axis runs over, the one named last changes fastest.
Arguments:
- recorded: float32 [4, 256, 256, 256], P('view', 'pencil'), may hold values from 0.5 to 4
- spectral_weight: float32 [4, 256, 256, 256], P('view', None, 'pencil'), may hold values from 0.05 to 1
- psf_taps: float32 [4, 3, 9], replicated, may hold values from 0.1 to 1
Outputs:
- joined_volume: float32 [256, 256, 256], P('pencil', 'view')
- estimate: float32 [256, 256, 256], P('pencil', 'view')
The draws below stay inside these ranges and needn't reach their ends.
All inputs are finite; a program needn't handle non-finite values.
Results may differ from the reference program's by a relative error of at most 0.00029.
Values sent between devices are 32-bit elements; how exact they have to be, the bound alone decides.
A program may use at most 192 MiB of HBM per device.

```python
import math
import jax
import jax.numpy as jnp
from jax import lax

NZ = 256
NY = 256
NX = 256
TAPS = 9
ITERS = 2
VIEWS = 4


def level_of(own_key, shape, pieces, low, top_value):
    level = 1.0
    for axis_at, blocks in pieces:
        draws = jax.random.uniform(jax.random.fold_in(jax.random.fold_in(own_key, 6), axis_at), (blocks,), jnp.float32, low / len(pieces), top_value / len(pieces))
        level = level * jnp.repeat(jnp.exp(draws), shape[axis_at] // blocks).reshape((-1,) + (1,) * (len(shape) - 1 - axis_at))
    return level


def setup_inputs(seed: int = 0) -> dict:
    arg_keys = jax.random.split(jax.random.key(seed), 4)
    return {
        "recorded": jnp.clip(jnp.exp(math.log(4.0) - 2.0794415 * jax.random.uniform(arg_keys[0], (VIEWS, NZ, NY, NX), jnp.float32) ** level_of(arg_keys[0], (VIEWS, NZ, NY, NX), ((0, 4), (1, 8)), -0.2, 0.2)), 0.5, 4.0),
        "spectral_weight": jnp.clip(jnp.exp(math.log(1.0) - 2.9957323 * jax.random.uniform(arg_keys[1], (VIEWS, NZ, NY, NX), jnp.float32) ** level_of(arg_keys[1], (VIEWS, NZ, NY, NX), ((0, 4), (2, 8)), -0.2, 0.2)), 0.05, 1.0),
        "psf_taps": jnp.clip(jnp.exp(jax.random.uniform(arg_keys[2], (VIEWS, 3, TAPS), jnp.float32, math.log(0.1), math.log(1.0))), 0.1, 1.0),
    }


def conv_along(field, column, axis_dim, margin):
    padding = [(0, 0)] * field.ndim
    padding[axis_dim] = (margin, margin)
    padded = jnp.pad(field, padding)
    length = field.shape[axis_dim]
    running = column[0] * lax.slice_in_dim(padded, 0, length, axis=axis_dim)
    for offset in range(1, column.shape[0]):
        running = running + column[offset] * lax.slice_in_dim(padded, offset, offset + length, axis=axis_dim)
    return running


def blur_field(field, kernel, margin):
    for axis_dim in range(3):
        field = conv_along(field, kernel[axis_dim], axis_dim, margin)
    return field


def reference(recorded, spectral_weight, psf_taps):
    combined = spectral_weight[0] * jnp.fft.fftn(recorded[0])
    for viewer in range(1, VIEWS):
        combined = combined + spectral_weight[viewer] * jnp.fft.fftn(recorded[viewer])
    joined_volume = jnp.real(jnp.fft.ifftn(combined)).astype(jnp.float32)
    kernels = psf_taps / jnp.sum(psf_taps, axis=-1, keepdims=True)
    margin = TAPS // 2
    estimate = 0.1 + jax.nn.softplus(joined_volume)
    for repeat in range(ITERS):
        summed = jnp.zeros_like(estimate)
        for viewer in range(VIEWS):
            blurred = blur_field(estimate, kernels[viewer], margin)
            ratio = recorded[viewer] / blurred
            summed = summed + blur_field(ratio, kernels[viewer][:, ::-1], margin)
        estimate = estimate * summed / VIEWS
    return joined_volume, estimate
```

```python
import math

import jax
import jax.numpy as jnp
from jax import lax
from jax.sharding import PartitionSpec as P

ITERS = 2
CHUNKS = 2


def padded_2(shard, sides, width):
    for axis, dim in sides:
        devices, length = (lax.axis_size(axis), shard.shape[dim])
        up = [(i, (i + 1) % devices) for i in range(devices - 1)]
        down = [(j, i) for i, j in up]
        last = lax.slice_in_dim(shard, length - width, length, axis=dim)
        leading = lax.slice_in_dim(shard, 0, width, axis=dim)
        before = lax.ppermute(last, axis, up)
        after = lax.ppermute(leading, axis, down)
        shard = jnp.concatenate([before, shard, after], axis=dim)
    return shard


def tables(length):
    positions = jnp.arange(length, dtype=jnp.int32)
    product = positions[:, None] * positions[None, :] % length
    phases = product.astype(jnp.float32) * (2.0 * math.pi / length)
    return (jnp.cos(phases), jnp.sin(phases))


def mix(form, left, right):
    return jnp.einsum(form, left, right, precision=lax.Precision.HIGH)


def folded(full, axis, dim, width):
    devices, length = (lax.axis_size(axis), full.shape[dim] - 2 * width)
    up = [(i, (i + 1) % devices) for i in range(devices - 1)]
    down = [(j, i) for i, j in up]
    before = lax.slice_in_dim(full, 0, width, axis=dim)
    after = lax.slice_in_dim(full, length + width, length + 2 * width, axis=dim)
    own = lax.slice_in_dim(full, width, length + width, axis=dim)
    from_below = lax.ppermute(after, axis, up)
    from_above = lax.ppermute(before, axis, down)
    spread = [(0, 0, 0)] * full.ndim
    spread[dim] = (0, length - width, 0)
    lower = lax.pad(from_below, jnp.float32(0), spread)
    spread[dim] = (length - width, 0, 0)
    return own + lower + lax.pad(from_above, jnp.float32(0), spread)


def band(taps, rows, columns, shift):
    offset = jnp.arange(columns)[None, :] - jnp.arange(rows)[:, None] + shift
    total = jnp.zeros((taps.shape[0], rows, columns), jnp.float32)
    for t in range(taps.shape[1]):
        total = total + jnp.where(offset == t, taps[:, t, None, None], 0.0)
    return total


def joined_of(slab, weights):
    view_count, view_index = lax.axis_size("view"), lax.axis_index("view")
    nx, ny = slab.shape[2], slab.shape[1]
    cos_x, sin_x = tables(nx)
    cos_y, sin_y = tables(ny)
    width = nx // CHUNKS
    sent = []
    for chunk in range(CHUNKS):
        part = slice(chunk * width, (chunk + 1) * width)
        real = mix("zyx,xk->zyk", slab, cos_x[:, part])
        imag = -mix("zyx,xk->zyk", slab, sin_x[:, part])
        out_real = mix("zyx,yk->zkx", real, cos_y) + mix("zyx,yk->zkx", imag, sin_y)
        out_imag = mix("zyx,yk->zkx", imag, cos_y) - mix("zyx,yk->zkx", real, sin_y)
        sent.append([
            lax.all_to_all(piece, "pencil", split_axis=1, concat_axis=0, tiled=True)
            for piece in (out_real, out_imag)
        ])
    inverse = []
    for chunk in range(CHUNKS):
        real, imag = sent[chunk]
        nz = real.shape[0]
        cos_z, sin_z = tables(nz)
        weight = weights[:, :, chunk * width:(chunk + 1) * width]
        out_real = weight * (mix("zyx,zk->kyx", real, cos_z) + mix("zyx,zk->kyx", imag, sin_z))
        out_imag = weight * (mix("zyx,zk->kyx", imag, cos_z) - mix("zyx,zk->kyx", real, sin_z))
        real = lax.psum_scatter(out_real, "view", scatter_dimension=1, tiled=True)
        imag = lax.psum_scatter(out_imag, "view", scatter_dimension=1, tiled=True)
        inverse.append((
            mix("kyx,kz->zyx", real, cos_z) - mix("kyx,kz->zyx", imag, sin_z),
            mix("kyx,kz->zyx", real, sin_z) + mix("kyx,kz->zyx", imag, cos_z),
        ))
    real = jnp.concatenate([pair[0] for pair in inverse], axis=2)
    imag = jnp.concatenate([pair[1] for pair in inverse], axis=2)
    rows = real.shape[1]
    moved = [
        lax.all_to_all(piece, "pencil", split_axis=0, concat_axis=1, tiled=True)
        for piece in (
            mix("zyk,kx->zyx", real, cos_x) - mix("zyk,kx->zyx", imag, sin_x),
            mix("zyk,kx->zyx", real, sin_x) + mix("zyk,kx->zyx", imag, cos_x),
        )
    ]
    scale = 1.0 / float(nz * ny * nx)
    held = [
        lax.dynamic_index_in_dim(
            table.reshape(-1, view_count, rows, ny), view_index, 1, keepdims=False
        ).reshape(-1, ny) * scale
        for table in (cos_y, sin_y)
    ]
    partial = mix("zkx,ky->zyx", moved[0], held[0]) - mix("zkx,ky->zyx", moved[1], held[1])
    return lax.psum_scatter(partial, "view", scatter_dimension=1, tiled=True)


def body(recorded, spectral_weight, psf_taps):
    view_count = lax.axis_size("view")
    joined_volume = joined_of(recorded[0], spectral_weight[0])
    kernels = psf_taps / jnp.sum(psf_taps, axis=-1, keepdims=True)
    margin = kernels.shape[-1] // 2
    stacked = lax.all_to_all(recorded, "view", split_axis=2, concat_axis=0, tiled=True)
    depth, rows, length = joined_volume.shape
    views = kernels.shape[0]
    blur_z = band(kernels[:, 0], depth, depth + 2 * margin, 0)
    blur_y = band(kernels[:, 1], rows, rows + 2 * margin, 0)
    blur_x = band(kernels[:, 2], length, length, margin)
    local = 0.1 + jax.nn.softplus(joined_volume)
    for repeat in range(ITERS):
        padded = padded_2(local, (("view", 1), ("pencil", 0)), margin)
        field = mix("vza,abx->vzbx", blur_z, padded)
        field = mix("vyb,vzbx->vzyx", blur_y, field)
        ratio = stacked / mix("vzyx,vcx->vzyc", field, blur_x)
        field = mix("vzyc,vcx->vzyx", ratio, blur_x)
        field = mix("vyb,vzyx->vzbx", blur_y, field)
        total = mix("vza,vzbx->abx", blur_z, field)
        total = folded(folded(total, "pencil", 0, margin), "view", 1, margin)
        local = local * total / view_count
    return (joined_volume, local)


def solution(mesh):
    return jax.shard_map(
        body,
        mesh=mesh,
        in_specs=(P("view", "pencil", None, None), P("view", None, "pencil", None), P()),
        out_specs=(P("pencil", "view", None), P("pencil", "view", None)),
        check_vma=False,
    )
```
